32 devices in a mesh: dp: 16 (over z, y, core), tensor: 2 (over x).
Axes of the slice: x: 2, y: 2, z: 4, core: 2. Of those that a mesh axis runs over, the one named last changes fastest.
Arguments:
- layer_input: bfloat16 [32768, 1024], P(('dp', 'tensor')), may hold values from -6 to 6
- gain_attn: bfloat16 [1024], P(('dp', 'tensor')), may hold values from 0.5 to 1.5
- w_query: bfloat16 [1024, 1024], P('dp', 'tensor'), may hold values from -0.1875 to 0.1875
- w_latent: bfloat16 [1024, 512], P('dp', 'tensor'), may hold values from -0.1875 to 0.1875
- w_key: bfloat16 [2, 256, 512], P('tensor', 'dp'), may hold values from -0.375 to 0.375
- w_value: bfloat16 [2, 256, 512], P('tensor', 'dp'), may hold values from -0.375 to 0.375
- w_output: bfloat16 [1024, 1024], P('tensor', 'dp'), may hold values from -2 to 2
- gain_ffn: bfloat16 [1024], P(('dp', 'tensor')), may hold values from 0.5 to 1.5
- w_gate: bfloat16 [1024, 2816], P('dp', 'tensor'), may hold values from -0.1875 to 0.1875
- w_up: bfloat16 [1024, 2816], P('dp', 'tensor'), may hold values from -0.1875 to 0.1875
- w_down: bfloat16 [2816, 1024], P('tensor', 'dp'), may hold values from -0.109375 to 0.109375
- parents: int32 [16, 13], P('dp'), may hold values from 0 to 4, as said below
- counts: int32 [16, 13], P('dp'), may hold values from 1 to 512, as said below
- upstream_grad: bfloat16 [32768, 1024], P(('dp', 'tensor')), may hold values from -6 to 6
Outputs:
- layer_out: bfloat16 [32768, 1024], P(('dp', 'tensor'))
- input_grad: float32 [32768, 1024], P(('dp', 'tensor'))
- gain_attn_grad: float32 [1024], P(('dp', 'tensor'))
- w_query_grad: float32 [1024, 1024], P('dp', 'tensor')
- w_latent_grad: float32 [1024, 512], P('dp', 'tensor')
- w_key_grad: float32 [2, 256, 512], P('tensor', 'dp')
- w_value_grad: float32 [2, 256, 512], P('tensor', 'dp')
- w_output_grad: float32 [1024, 1024], P('tensor', 'dp')
- gain_ffn_grad: float32 [1024], P(('dp', 'tensor'))
- w_gate_grad: float32 [1024, 2816], P('dp', 'tensor')
- w_up_grad: float32 [1024, 2816], P('dp', 'tensor')
- w_down_grad: float32 [2816, 1024], P('tensor', 'dp')
- rms_stats: float32 [3], replicated
The draws below stay inside these ranges and needn't reach their ends.
Inputs may be any that keep to these rules, and one draw needn't show every extreme that they name: `parents`: segment 0 is the trunk and names itself, the 4 branches (segments 1 to 4) name segment 0, and each of the 8 leaves names one of the branches. `counts`: A segment's count lies between 1 and its length (512 for the trunk, 128 otherwise); the valid tokens of a segment are its first ones.
All inputs are finite; a program needn't handle non-finite values.
Results may differ from the reference program's by a relative error of at most 0.018.
Values may be sent and summed in bfloat16 or wider, within the bound.
A program may use at most 320 MiB of HBM per device.

```python
import jax
import jax.numpy as jnp
from jax import lax

D = 1024
HQ = 16
E = 64
G = 2
L = 256
FF = 2816
TRUNK = 512
SEG = 128
NBRANCH = 4
NLEAF = 8
NSEG = 13
TREE = 2048
TREES = 16
TOKENS = 32768


def draw_parents(key, part):
    leaf_parent = jax.random.randint(key, (TREES, NLEAF), 1, NBRANCH + 1)
    chosen = jax.random.randint(jax.random.fold_in(key, 7), (TREES, 1), 0, NLEAF)
    leaf_parent = jnp.where(jnp.arange(NLEAF)[None, :] == chosen, NBRANCH, leaf_parent)
    head_part = jnp.zeros((TREES, 1 + NBRANCH), jnp.int32)
    return jnp.concatenate([head_part, leaf_parent.astype(jnp.int32)], axis=1).astype(jnp.int32)


def draw_counts(key, part):
    seg_ids = jnp.arange(NSEG)
    seg_length = jnp.where(seg_ids == 0, TRUNK, SEG)
    drawn = jax.random.randint(key, (TREES, NSEG), 1, seg_length[None, :] + 1)
    tree_ids = jnp.arange(TREES)[:, None]
    drawn = jnp.where((tree_ids == 0) & (seg_ids[None, :] == 0), TRUNK, drawn)
    drawn = jnp.where((tree_ids == 0) & (seg_ids[None, :] == NSEG - 1), 1, drawn)
    return drawn.astype(jnp.int32)


def levels(stream_key, dims, pieces, least, high):
    def one(dim, shards_of):
        draws = jax.random.uniform(jax.random.fold_in(jax.random.fold_in(stream_key, 6), dim), (shards_of,), jnp.float32, least / len(pieces), high / len(pieces))
        return jnp.repeat(jnp.exp(draws), dims[dim] // shards_of).reshape((-1,) + (1,) * (len(dims) - dim - 1))

    level = one(*pieces[0])
    for cut in pieces[1:]:
        level = level * one(*cut)
    return level


def centred(stream_key, shape, deviation, most, cuts=(), kind=jnp.bfloat16):
    factor_of = levels(stream_key, shape, cuts, -0.22, 0.18) if cuts else 1.0
    values = jax.random.normal(stream_key, shape, jnp.float32) * deviation * factor_of
    return jnp.minimum(jnp.maximum(values, -most), most).astype(kind)


def setup_inputs(seed: int = 0) -> dict:
    key_of = jax.random.split(jax.random.key(seed), 15)
    return {
        "layer_input": centred(key_of[0], (TOKENS, D), 1.0, 6.0, ((0, 32),)),
        "gain_attn": jnp.clip(1.0 + 0.1 * jax.random.normal(key_of[1], (D,), jnp.float32), 0.5, 1.5).astype(jnp.bfloat16),
        "w_query": centred(key_of[2], (D, HQ * E), D ** -0.5, 0.1875, ((0, 16), (1, 2))),
        "w_latent": centred(key_of[3], (D, G * L), D ** -0.5, 0.1875, ((0, 16), (1, 2))),
        "w_key": centred(key_of[4], (G, L, HQ // G * E), L ** -0.5, 0.375, ((0, 2), (1, 16))),
        "w_value": centred(key_of[5], (G, L, HQ // G * E), L ** -0.5, 0.375, ((0, 2), (1, 16))),
        "w_output": centred(key_of[6], (HQ * E, D), (max(HQ * E // 128, 1)) ** -0.5, 2.0, ((0, 2), (1, 16))),
        "gain_ffn": jnp.clip(1.0 + 0.1 * jax.random.normal(key_of[7], (D,), jnp.float32), 0.5, 1.5).astype(jnp.bfloat16),
        "w_gate": centred(key_of[8], (D, FF), D ** -0.5, 0.1875, ((0, 16), (1, 2))),
        "w_up": centred(key_of[9], (D, FF), D ** -0.5, 0.1875, ((0, 16), (1, 2))),
        "w_down": centred(key_of[10], (FF, D), FF ** -0.5, 0.109375, ((0, 2), (1, 16))),
        "parents": draw_parents(jax.random.fold_in(key_of[14], 71), 0),
        "counts": draw_counts(jax.random.fold_in(key_of[14], 71), 0),
        "upstream_grad": centred(key_of[13], (TOKENS, D), 1.0, 6.0, ((0, 32),)),
    }


@jax.custom_vjp
def low(v):
    return lax.optimization_barrier(v.astype(jnp.bfloat16)).astype(jnp.float32)

@jax.custom_vjp
def low_back(v):
    return v

def low_keep(v):
    return (low(v), None)

def low_pass(kept, grad):
    return (grad,)

def back_keep(v):
    return (v, None)

def back_low(kept, grad):
    return (low(grad),)
low.defvjp(low_keep, low_pass)
low_back.defvjp(back_keep, back_low)
EPSILON = 1e-06
HIGH = lax.Precision.HIGHEST

def matmul(left, right):
    return jnp.dot(left, right, precision=HIGH, preferred_element_type=jnp.float32)

def rms_norm(inputs):
    return inputs * lax.rsqrt(lax.optimization_barrier(jnp.mean(inputs * inputs, axis=-1, keepdims=True)) + EPSILON)

def token_tables(parents_row, counts_row, tree_len):
    position = jnp.arange(tree_len, dtype=jnp.int32)
    beyond = position - TRUNK
    segment = jnp.where(position < TRUNK, 0, 1 + beyond // SEG).astype(jnp.int32)
    offset = jnp.where(position < TRUNK, position, beyond % SEG).astype(jnp.int32)
    seg_ids = jnp.arange(NSEG, dtype=jnp.int32)
    seg_hot = segment[:, None] == seg_ids[None, :]
    seg_limit = lax.optimization_barrier(jnp.sum(jnp.where(seg_hot, counts_row[None, :], 0), axis=1))
    valid_tok = offset < seg_limit
    parent_hot = (parents_row[:, None] == seg_ids[None, :]).astype(jnp.float32)
    ancestor = jnp.eye(NSEG, dtype=jnp.float32) + parent_hot + matmul(parent_hot, parent_hot) > 0.5
    key_ok = matmul(ancestor.astype(jnp.float32), seg_hot.astype(jnp.float32).T) * valid_tok.astype(jnp.float32)[None, :]
    return (segment, offset, valid_tok, key_ok, seg_hot)

def allowed_rows(segment, offset, key_ok, seg_hot, first_row, block_len):
    seg_rows = lax.dynamic_slice_in_dim(segment, first_row, block_len)
    off_rows = lax.dynamic_slice_in_dim(offset, first_row, block_len)
    hot_rows = lax.dynamic_slice_in_dim(seg_hot, first_row, block_len).astype(jnp.float32)
    reach = matmul(hot_rows, key_ok) > 0.5
    order = (seg_rows[:, None] != segment[None, :]) | (offset[None, :] <= off_rows[:, None])
    return reach & order

def attend(query_block, mask_block, key_heads, value_heads):
    scores = low_back(jnp.einsum('qhe,khe->hqk', query_block, key_heads, precision=HIGH) * E ** (-0.5))
    scores = jnp.where(mask_block[None], scores, -1e+30)
    shifted = jnp.exp(scores - lax.optimization_barrier(jnp.max(scores, axis=-1, keepdims=True)))
    attn_probs = low(shifted / lax.optimization_barrier(jnp.sum(shifted, axis=-1, keepdims=True)))
    return jnp.einsum('hqk,khe->qhe', attn_probs, value_heads, precision=HIGH)

def decoder_layer(inputs, weights, mask_blocks):
    gain_attn, w_query, w_latent, w_key, w_value, w_output, gain_ffn, w_gate, w_up, w_down = weights
    block_len = min(512, TREE)
    normed_attn = low(rms_norm(inputs) * gain_attn)
    query_flat = low_back(low(matmul(normed_attn, w_query)))
    latent = low_back(low(matmul(normed_attn, w_latent)))
    latent_groups = latent.reshape(TREE, G, L)
    key_heads = low_back(low(jnp.einsum('tgl,glf->tgf', latent_groups, w_key, precision=HIGH))).reshape(TREE, HQ, E)
    value_heads = low_back(low(jnp.einsum('tgl,glf->tgf', latent_groups, w_value, precision=HIGH))).reshape(TREE, HQ, E)
    query_blocks = query_flat.reshape(TREE // block_len, block_len, HQ, E)
    attend_saved = jax.checkpoint(attend)
    mixed_out = lax.map(lambda step_item: attend_saved(step_item[0], step_item[1], key_heads, value_heads), (query_blocks, mask_blocks))
    heads_out = low_back(low(mixed_out.reshape(TREE, HQ * E)))
    branch = low_back(matmul(heads_out, w_output))
    residual = inputs + branch
    normed_ffn = low(rms_norm(residual) * gain_ffn)
    gate_pre = low_back(matmul(normed_ffn, w_gate))
    up_proj = low_back(matmul(normed_ffn, w_up))
    hidden = low(jax.nn.silu(gate_pre) * up_proj)
    ffn_out = matmul(hidden, w_down)
    return (residual + ffn_out, (branch, residual, ffn_out))

def reference(layer_input, gain_attn, w_query, w_latent, w_key, w_value, w_output, gain_ffn, w_gate, w_up, w_down, parents, counts, upstream_grad):
    weights = tuple((weight.astype(jnp.float32) for weight in (gain_attn, w_query, w_latent, w_key, w_value, w_output, gain_ffn, w_gate, w_up, w_down)))
    block_len = min(512, TREE)
    inputs_all = layer_input.astype(jnp.float32).reshape(TREES, TREE, D)
    grads_all = upstream_grad.astype(jnp.float32).reshape(TREES, TREE, D)

    def per_tree(accumulators, step_item):
        inputs_tree, grad_tree, parents_row, counts_row = step_item
        segment, offset, valid_tok, key_ok, seg_hot = token_tables(parents_row, counts_row, TREE)
        allowed = allowed_rows(segment, offset, key_ok, seg_hot, 0, TREE).reshape(TREE // block_len, block_len, TREE)
        outputs, pullback, aux_values = jax.vjp(lambda inputs_now, weights_now: decoder_layer(inputs_now, weights_now, allowed), inputs_tree, weights, has_aux=True)
        input_grad, weight_grads = pullback(grad_tree)
        valid_rows = valid_tok.astype(jnp.float32)[:, None]
        totals = jnp.stack([jnp.sum(valid_rows * section * section) for section in aux_values] + [jnp.sum(valid_rows)])
        weight_sum, stat_sum = accumulators
        updated = (jax.tree.map(jnp.add, weight_sum, weight_grads), stat_sum + totals)
        return (updated, (outputs.astype(jnp.bfloat16), input_grad))
    initial = (tuple((jnp.zeros_like(weight) for weight in weights)), jnp.zeros((4,), jnp.float32))
    (weight_sum, stat_sum), (layer_out, input_grad) = lax.scan(per_tree, initial, (inputs_all, grads_all, parents, counts))
    rms_stats = jnp.sqrt(stat_sum[:3] / (stat_sum[3] * D))
    return (layer_out.reshape(TOKENS, D), input_grad.reshape(TOKENS, D), weight_sum[0], weight_sum[1], weight_sum[2], weight_sum[3], weight_sum[4], weight_sum[5], weight_sum[6], weight_sum[7], weight_sum[8], weight_sum[9], rms_stats)
```

```python
import jax
import jax.numpy as jnp
from jax import lax
from jax.experimental import pallas as pl
from jax.experimental.pallas import tpu as pltpu
from jax.sharding import PartitionSpec as P

E = 64
TRUNK = 512
SEG = 128
NSEG = 13
NBRANCH = 4
PAIR = 2 * E
CHUNK = 256
NEG = -1e30
EPSILON = 1e-06

GATHER_AXES = ("tensor", "dp")

NN = (((1,), (0,)), ((), ()))
NT = (((1,), (1,)), ((), ()))
TN = (((0,), (0,)), ((), ()))


def mm(left, right, dims=NN):
    return lax.dot_general(left, right, dims, preferred_element_type=jnp.float32)


def block_scalars(meta_ref, block):
    leaf_side = meta_ref[0] == 1
    segment = jnp.where(leaf_side, block + (1 + NBRANCH), block - (TRUNK // SEG - 1))
    present = segment >= 1
    index = jnp.maximum(segment, 0)
    parent = meta_ref[1 + NSEG + index]
    own_count = jnp.where(present, meta_ref[1 + index], 0)
    parent_count = jnp.where(present & (parent >= 1), meta_ref[1 + parent], 0)
    parent_row = TRUNK + SEG * jnp.maximum(parent - 1, 0)
    return own_count, parent_count, pl.multiple_of(parent_row, SEG)


def trunk_limits(meta_ref, step):
    causal = (meta_ref[0] == 0) & (step < TRUNK // CHUNK)
    return meta_ref[1], jnp.where(causal, step * CHUNK, TRUNK)


def head_masks(dtype, value):
    lane = lax.broadcasted_iota(jnp.int32, (1, PAIR), 1)
    first = jnp.where(lane < E, value, 0.0).astype(dtype)
    second = jnp.where(lane < E, 0.0, value).astype(dtype)
    return first, second


def forward_kernel(meta_ref, q_ref, kv_ref, o_ref, lse_ref):
    step = pl.program_id(1)
    local_rows = kv_ref.shape[0] // 2
    query = q_ref[...]
    scale = head_masks(query.dtype, E ** (-0.5))
    trunk_count, shift = trunk_limits(meta_ref, step)
    key_pos = lax.broadcasted_iota(jnp.int32, (CHUNK, TRUNK), 1)
    row_pos = lax.broadcasted_iota(jnp.int32, (CHUNK, TRUNK), 0)
    trunk_ok = (key_pos <= row_pos + shift) & (key_pos < trunk_count)
    seg_key = lax.broadcasted_iota(jnp.int32, (SEG, SEG), 1)
    seg_row = lax.broadcasted_iota(jnp.int32, (SEG, SEG), 0)
    starts, par_ok, own_ok = [], [], []
    for j in range(CHUNK // SEG):
        block = step * (CHUNK // SEG) + j
        own_count, parent_count, parent_row = block_scalars(meta_ref, block)
        starts.append((parent_row, pl.multiple_of(local_rows + block * SEG, SEG)))
        par_ok.append(seg_key < parent_count)
        own_ok.append((seg_key <= seg_row) & (seg_key < own_count))
    outs, lses = [], []
    for h in range(2):
        qh = query * scale[h]
        trunk = jnp.where(trunk_ok, mm(qh, kv_ref[0:TRUNK, 0:PAIR], NT), NEG)
        par, own = [], []
        for j, (first, second) in enumerate(starts):
            qj = qh[j * SEG : (j + 1) * SEG]
            par.append(jnp.where(par_ok[j], mm(qj, kv_ref[pl.ds(first, SEG), 0:PAIR], NT), NEG))
            own.append(jnp.where(own_ok[j], mm(qj, kv_ref[pl.ds(second, SEG), 0:PAIR], NT), NEG))
        par_all = jnp.concatenate(par, axis=0)
        own_all = jnp.concatenate(own, axis=0)
        top = jnp.maximum(par_all, own_all)
        for i in range(TRUNK // SEG):
            top = jnp.maximum(top, trunk[:, i * SEG : (i + 1) * SEG])
        top = jnp.max(top, axis=1, keepdims=True)
        trunk = jnp.exp(trunk - top)
        par_all = jnp.exp(par_all - top)
        own_all = jnp.exp(own_all - top)
        total = par_all + own_all
        for i in range(TRUNK // SEG):
            total = total + trunk[:, i * SEG : (i + 1) * SEG]
        total = jnp.sum(total, axis=1, keepdims=True)
        out = mm(trunk.astype(jnp.bfloat16), kv_ref[0:TRUNK, PAIR : 2 * PAIR])
        tails = []
        for j, (first, second) in enumerate(starts):
            part = slice(j * SEG, (j + 1) * SEG)
            tails.append(
                mm(par_all[part].astype(jnp.bfloat16), kv_ref[pl.ds(first, SEG), PAIR : 2 * PAIR])
                + mm(own_all[part].astype(jnp.bfloat16), kv_ref[pl.ds(second, SEG), PAIR : 2 * PAIR])
            )
        out = out + jnp.concatenate(tails, axis=0)
        outs.append(out * (1.0 / total))
        lses.append(jnp.broadcast_to(top + jnp.log(total), (CHUNK, PAIR)))
    lane = lax.broadcasted_iota(jnp.int32, (CHUNK, PAIR), 1)
    o_ref[...] = jnp.where(lane < E, outs[0], outs[1]).astype(o_ref.dtype)
    turned = jnp.transpose(jnp.where(lane < E, lses[0], lses[1]))
    lse_ref[0, 0:1, :] = turned[0:1, :]
    lse_ref[0, 1:2, :] = turned[E : E + 1, :]


def attend_forward(meta, query, kv):
    rows, width = query.shape
    pairs = width // PAIR
    return pl.pallas_call(
        forward_kernel,
        grid_spec=pltpu.PrefetchScalarGridSpec(
            num_scalar_prefetch=1,
            grid=(pairs, rows // CHUNK),
            in_specs=[
                pl.BlockSpec((CHUNK, PAIR), lambda p, c, meta: (c, p)),
                pl.BlockSpec((2 * rows, 2 * PAIR), lambda p, c, meta: (0, p)),
            ],
            out_specs=[
                pl.BlockSpec((CHUNK, PAIR), lambda p, c, meta: (c, p)),
                pl.BlockSpec((1, 2, CHUNK), lambda p, c, meta: (p, 0, c)),
            ],
        ),
        out_shape=[
            jax.ShapeDtypeStruct((rows, width), jnp.bfloat16),
            jax.ShapeDtypeStruct((pairs, 2, rows), jnp.float32),
        ],
        name="attend_forward",
    )(meta, query, kv)


def backward_kernel(meta_ref, q_ref, kv_ref, o_ref, do_ref, lse_ref, dq_ref, dkv_ref, acc_ref):
    step = pl.program_id(1)
    local_rows = kv_ref.shape[0] // 2

    @pl.when(step == 0)
    def _():
        acc_ref[...] = jnp.zeros_like(acc_ref)

    query = q_ref[...]
    grad = do_ref[...]
    scale = head_masks(query.dtype, E ** (-0.5))
    keep = head_masks(query.dtype, 1.0)
    product = jnp.transpose(grad.astype(jnp.float32) * o_ref[...].astype(jnp.float32))
    trunk_count, shift = trunk_limits(meta_ref, step)
    key_pos = lax.broadcasted_iota(jnp.int32, (TRUNK, CHUNK), 0)
    row_pos = lax.broadcasted_iota(jnp.int32, (TRUNK, CHUNK), 1)
    trunk_ok = (key_pos <= row_pos + shift) & (key_pos < trunk_count)
    seg_key = lax.broadcasted_iota(jnp.int32, (SEG, SEG), 0)
    seg_row = lax.broadcasted_iota(jnp.int32, (SEG, SEG), 1)
    blocks = []
    for j in range(CHUNK // SEG):
        block = step * (CHUNK // SEG) + j
        own_count, parent_count, parent_row = block_scalars(meta_ref, block)
        own_row = pl.multiple_of(local_rows + block * SEG, SEG)
        blocks.append(
            (
                (parent_row, seg_key < parent_count),
                (own_row, (seg_key <= seg_row) & (seg_key < own_count)),
            )
        )
    query_grads = []
    trunk_parts = []
    block_parts = [[[], []] for _ in blocks]
    for h in range(2):
        qh = query * scale[h]
        gh = grad * keep[h]
        lse = lse_ref[0, h : h + 1, :]
        inner = jnp.sum(product[h * E : (h + 1) * E], axis=0, keepdims=True)

        def part(rows, allowed, qs, gs, lse_row, inner_row):
            keys = kv_ref[rows, 0:PAIR]
            values = kv_ref[rows, PAIR : 2 * PAIR]
            scores = jnp.where(allowed, mm(keys, qs, NT), NEG)
            probs = jnp.exp(scores - lse_row)
            score_grad = (probs * (mm(values, gs, NT) - inner_row)).astype(jnp.bfloat16)
            return (
                mm(score_grad, keys, TN),
                mm(score_grad, qs),
                mm(probs.astype(jnp.bfloat16), gs),
            )

        query_grad, key_part, value_part = part(slice(0, TRUNK), trunk_ok, qh, gh, lse, inner)
        trunk_parts.append((key_part, value_part))
        tails = []
        for j, sources in enumerate(blocks):
            cut = slice(j * SEG, (j + 1) * SEG)
            tail = 0.0
            for k, (first, allowed) in enumerate(sources):
                moved, key_part, value_part = part(
                    pl.ds(first, SEG), allowed, qh[cut], gh[cut], lse[:, cut], inner[:, cut]
                )
                tail = tail + moved
                block_parts[j][k].append((key_part, value_part))
            tails.append(tail)
        query_grads.append(query_grad + jnp.concatenate(tails, axis=0))
    lane = lax.broadcasted_iota(jnp.int32, (CHUNK, PAIR), 1)
    dq_ref[...] = (jnp.where(lane < E, query_grads[0], query_grads[1]) * E ** (-0.5)).astype(
        dq_ref.dtype
    )
    for side in range(2):
        cols = slice(side * PAIR, (side + 1) * PAIR)
        acc_ref[0:TRUNK, cols] += trunk_parts[0][side] + trunk_parts[1][side]
        for j, sources in enumerate(blocks):
            for k, (first, _) in enumerate(sources):
                both = block_parts[j][k][0][side] + block_parts[j][k][1][side]
                if k == 0:
                    acc_ref[pl.ds(first, SEG), cols] += both
                else:
                    dkv_ref[pl.ds(first, SEG), cols] = both.astype(dkv_ref.dtype)

    @pl.when(step == pl.num_programs(1) - 1)
    def _():
        dkv_ref[0:local_rows, :] = acc_ref[...].astype(dkv_ref.dtype)


def attend_backward(meta, query, kv, out, grad, lse):
    rows, width = query.shape
    pairs = width // PAIR
    row_spec = pl.BlockSpec((CHUNK, PAIR), lambda p, c, meta: (c, p))
    kv_spec = pl.BlockSpec((2 * rows, 2 * PAIR), lambda p, c, meta: (0, p))
    return pl.pallas_call(
        backward_kernel,
        grid_spec=pltpu.PrefetchScalarGridSpec(
            num_scalar_prefetch=1,
            grid=(pairs, rows // CHUNK),
            in_specs=[
                row_spec,
                kv_spec,
                row_spec,
                row_spec,
                pl.BlockSpec((1, 2, CHUNK), lambda p, c, meta: (p, 0, c)),
            ],
            out_specs=[row_spec, kv_spec],
            scratch_shapes=[pltpu.VMEM((rows, 2 * PAIR), jnp.float32)],
        ),
        out_shape=[
            jax.ShapeDtypeStruct((rows, width), jnp.bfloat16),
            jax.ShapeDtypeStruct((2 * rows, 2 * width), jnp.bfloat16),
        ],
        name="attend_backward",
    )(meta, query, kv, out, grad, lse)


def norm_stats(inputs):
    inverse = lax.rsqrt(jnp.mean(inputs * inputs, axis=-1, keepdims=True) + EPSILON)
    return (inputs * inverse, inverse)


def norm_back(normed_grad, gain_vec, normed, inverse):
    scaled = normed_grad * gain_vec
    inner = jnp.mean(scaled * normed, axis=-1, keepdims=True)
    return (inverse * (scaled - normed * inner), jnp.sum(normed_grad * normed, axis=0))


def interleave(keys, values):
    rows, width = keys.shape
    shape = (rows, width // PAIR, 1, PAIR)
    both = jnp.concatenate([keys.reshape(shape), values.reshape(shape)], axis=2)
    return both.reshape(rows, 2 * width)


def scatter(parts):
    return lax.psum_scatter(
        jnp.concatenate(parts, axis=0), GATHER_AXES, scatter_dimension=0, tiled=True
    )


def local(
    layer_input,
    gain_attn,
    w_query,
    w_latent,
    w_key,
    w_value,
    w_output,
    gain_ffn,
    w_gate,
    w_up,
    w_down,
    parents,
    counts,
    upstream_grad,
):
    bf16 = jnp.bfloat16
    row_count, model_width = layer_input.shape
    sides = lax.axis_size("tensor")
    dp_size = lax.axis_size("dp")
    side = lax.axis_index("tensor")
    shard_rows, query_len = w_query.shape
    latent_len = w_latent.shape[1]
    hidden_len = w_gate.shape[1]
    kv_rows, kv_len = w_key.shape[1:]
    gain_len = gain_attn.shape[0]
    kv_cols = kv_rows * 2 * kv_len // shard_rows
    gain_cols = 2 * E

    meta = jnp.concatenate([side[None].astype(jnp.int32), counts[0], parents[0]])

    sent = lax.ppermute(layer_input, "tensor", [(0, 1)])

    gain_row = jnp.concatenate([gain_attn, gain_ffn])[None, :]
    gain_block = jnp.pad(gain_row, ((0, shard_rows - 1), (0, gain_cols - 2 * gain_len)))
    attn_pack = jnp.concatenate(
        [
            w_query,
            w_latent,
            w_output.T,
            interleave(w_key[0], w_value[0]).reshape(shard_rows, kv_cols),
            gain_block,
        ],
        axis=1,
    )
    attn_all = lax.all_gather(attn_pack, GATHER_AXES, axis=0, tiled=True)
    gate_up_all = lax.all_gather(
        jnp.concatenate([w_gate, w_up], axis=1), GATHER_AXES, axis=0, tiled=True
    )
    down_all = lax.all_gather(w_down.T, GATHER_AXES, axis=0, tiled=True)

    def part_of(gathered, t, first, size):
        return lax.slice(
            gathered, (t * model_width, first), ((t + 1) * model_width, first + size)
        )

    first_latent = query_len
    first_out = first_latent + latent_len
    first_kv = first_out + query_len
    first_gain = first_kv + kv_cols
    query_w = [part_of(attn_all, t, 0, query_len) for t in range(sides)]
    latent_w = [part_of(attn_all, t, first_latent, latent_len) for t in range(sides)]
    out_w = [part_of(attn_all, t, first_out, query_len) for t in range(sides)]
    kv_w = [
        part_of(attn_all, t, first_kv, kv_cols).reshape(dp_size * kv_rows, 2 * kv_len)
        for t in range(sides)
    ]
    gains = attn_all[:, first_gain : first_gain + 2 * gain_len]
    gains = gains.reshape(sides, dp_size, shard_rows, 2, gain_len)[:, :, 0]
    gains = gains.transpose(2, 1, 0, 3).reshape(2, model_width).astype(jnp.float32)
    gain_one, gain_two = gains[0], gains[1]
    gate_w = [part_of(gate_up_all, t, 0, hidden_len) for t in range(sides)]
    up_w = [part_of(gate_up_all, t, hidden_len, hidden_len) for t in range(sides)]
    down_w = [part_of(down_all, t, 0, hidden_len) for t in range(sides)]

    context_input = jnp.where(side == 0, layer_input, sent)
    inputs = layer_input.astype(jnp.float32)
    normed_one, inverse_one = norm_stats(inputs)
    attn_in = (normed_one * gain_one).astype(bf16)
    context_in = (norm_stats(context_input.astype(jnp.float32))[0] * gain_one).astype(bf16)
    both_in = jnp.concatenate([context_in, attn_in], axis=0)
    queries, latents, kvs, heads, lses = [], [], [], [], []
    for t in range(sides):
        latents.append(mm(both_in, latent_w[t]).astype(bf16))
        queries.append(mm(attn_in, query_w[t]).astype(bf16))
        kvs.append(mm(latents[t], kv_w[t]).astype(bf16))
        out, lse = attend_forward(meta, queries[t], kvs[t])
        heads.append(out)
        lses.append(lse)
    branch = sum(mm(heads[t], out_w[t], NT) for t in range(sides))
    residual = inputs + branch
    normed_two, inverse_two = norm_stats(residual)
    ffn_in = (normed_two * gain_two).astype(bf16)

    gates = [mm(ffn_in, gate_w[t]) for t in range(sides)]
    ups = [mm(ffn_in, up_w[t]) for t in range(sides)]
    sigs = [jax.nn.sigmoid(gate) for gate in gates]
    hiddens = [(gates[t] * sigs[t] * ups[t]).astype(bf16) for t in range(sides)]
    ffn_out = sum(mm(hiddens[t], down_w[t], NT) for t in range(sides))
    final_out = (residual + ffn_out).astype(bf16)
    down_grads = [mm(upstream_grad, hiddens[t], TN).astype(bf16) for t in range(sides)]
    down_sum = scatter(down_grads)

    position = side * row_count + lax.broadcasted_iota(jnp.int32, (row_count, NSEG), 0)
    seg_ids = lax.broadcasted_iota(jnp.int32, (row_count, NSEG), 1)
    beyond = position - TRUNK
    segment = jnp.where(beyond < 0, 0, 1 + beyond // SEG)
    offset = jnp.where(beyond < 0, position, beyond % SEG)
    valid = jnp.any((segment == seg_ids) & (offset < counts[0][None, :]), axis=1, keepdims=True)
    valid = valid.astype(jnp.float32)
    stat_terms = jnp.stack(
        [
            jnp.sum(valid * branch * branch),
            jnp.sum(valid * residual * residual),
            jnp.sum(valid * ffn_out * ffn_out),
            jnp.sum(valid),
        ]
    )
    stat_rows = jnp.broadcast_to(jnp.pad(stat_terms, (0, 2 * E - 4))[None, :], (8, 2 * E))
    stat_all = lax.all_gather(stat_rows, GATHER_AXES, axis=0, tiled=True)
    stat_totals = jnp.sum(stat_all.reshape(sides * dp_size, 8, 2 * E)[:, 0, :4], axis=0)
    rms_stats = jnp.sqrt(stat_totals[:3] / (stat_totals[3] * model_width))

    ffn_grads = []
    normed_grad_two = 0.0
    for t in range(sides):
        hidden_grad = mm(upstream_grad, down_w[t])
        gate_act = gates[t] * sigs[t]
        gate_grad = (
            hidden_grad * ups[t] * sigs[t] * (1.0 + gates[t] * (1.0 - sigs[t]))
        ).astype(bf16)
        up_grad = (hidden_grad * gate_act).astype(bf16)
        normed_grad_two = (
            normed_grad_two + mm(gate_grad, gate_w[t], NT) + mm(up_grad, up_w[t], NT)
        )
        ffn_grads.append((mm(ffn_in, gate_grad, TN).astype(bf16), mm(ffn_in, up_grad, TN).astype(bf16)))
    gate_sum = scatter([pair[0] for pair in ffn_grads])
    up_sum = scatter([pair[1] for pair in ffn_grads])
    residual_part, gain_two_grad = norm_back(normed_grad_two, gain_two, normed_two, inverse_two)
    residual_grad = upstream_grad.astype(jnp.float32) + residual_part
    branch_grad = residual_grad.astype(bf16)

    attn_grads = []
    normed_grad_one = 0.0
    for t in range(sides):
        out_grad = mm(branch_grad, heads[t], TN).astype(bf16)
        heads_grad = mm(branch_grad, out_w[t]).astype(bf16)
        query_grad, kv_grad = attend_backward(
            meta, queries[t], kvs[t], heads[t], heads_grad, lses[t]
        )
        latent_part = mm(kv_grad, kv_w[t], NT)
        context_part = latent_part[:row_count]
        returned = lax.ppermute(context_part.astype(bf16), "tensor", [(1, 0)])
        kv_w_grad = mm(latents[t], kv_grad, TN).astype(bf16)
        query_w_grad = mm(attn_in, query_grad, TN).astype(bf16)
        latent_grad = (
            latent_part[row_count:]
            + jnp.where(side == 0, context_part, 0.0)
            + returned.astype(jnp.float32)
        ).astype(bf16)
        latent_w_grad = mm(attn_in, latent_grad, TN).astype(bf16)
        normed_grad_one = (
            normed_grad_one + mm(query_grad, query_w[t], NT) + mm(latent_grad, latent_w[t], NT)
        )
        attn_grads.append(
            [query_w_grad, latent_w_grad, out_grad, kv_w_grad.reshape(model_width, kv_cols)]
        )
    input_part, gain_one_grad = norm_back(normed_grad_one, gain_one, normed_one, inverse_one)
    input_grad = residual_grad + input_part

    gain_grads = jnp.stack([gain_one_grad, gain_two_grad]).reshape(2, dp_size, sides, gain_len)
    gain_grads = gain_grads.transpose(2, 1, 0, 3).reshape(sides, dp_size, 1, 2 * gain_len)
    gain_grads = jnp.pad(
        gain_grads.astype(bf16),
        ((0, 0), (0, 0), (0, shard_rows - 1), (0, gain_cols - 2 * gain_len)),
    ).reshape(sides, model_width, gain_cols)
    attn_sum = scatter(
        [jnp.concatenate(attn_grads[t] + [gain_grads[t]], axis=1) for t in range(sides)]
    ).astype(jnp.float32)
    kv_sum = attn_sum[:, first_kv:first_gain].reshape(kv_rows, kv_len // PAIR, 2, PAIR)
    return (
        final_out,
        input_grad,
        attn_sum[0, first_gain : first_gain + gain_len],
        attn_sum[:, :query_len],
        attn_sum[:, first_latent:first_out],
        kv_sum[:, :, 0].reshape(1, kv_rows, kv_len),
        kv_sum[:, :, 1].reshape(1, kv_rows, kv_len),
        attn_sum[:, first_out:first_kv].T,
        attn_sum[0, first_gain + gain_len : first_gain + 2 * gain_len],
        gate_sum.astype(jnp.float32),
        up_sum.astype(jnp.float32),
        down_sum.astype(jnp.float32).T,
        rms_stats,
    )


def solution(mesh):
    placed = (
        P(("dp", "tensor"), None),
        P(("dp", "tensor")),
        P("dp", "tensor"),
        P("dp", "tensor"),
        P("tensor", "dp", None),
        P("tensor", "dp", None),
        P("tensor", "dp"),
        P(("dp", "tensor")),
        P("dp", "tensor"),
        P("dp", "tensor"),
        P("tensor", "dp"),
        P("dp", None),
        P("dp", None),
        P(("dp", "tensor"), None),
    )
    return jax.shard_map(
        local,
        mesh=mesh,
        in_specs=placed,
        out_specs=(
            P(("dp", "tensor"), None),
            P(("dp", "tensor"), None),
            P(("dp", "tensor")),
            P("dp", "tensor"),
            P("dp", "tensor"),
            P("tensor", "dp", None),
            P("tensor", "dp", None),
            P("tensor", "dp"),
            P(("dp", "tensor")),
            P("dp", "tensor"),
            P("dp", "tensor"),
            P("tensor", "dp"),
            P(),
        ),
        check_vma=False,
    )
```

```python
import jax
import jax.numpy as jnp
from jax import lax
from jax.experimental import pallas as pl
from jax.experimental.pallas import tpu as pltpu
from jax.sharding import PartitionSpec as P

E = 64
TRUNK = 512
SEG = 128
NSEG = 13
NBRANCH = 4
PAIR = 2 * E
CHUNK = 256
NEG = -1e30
EPSILON = 1e-06

GATHER_AXES = ("tensor", "dp")

NN = (((1,), (0,)), ((), ()))
NT = (((1,), (1,)), ((), ()))
TN = (((0,), (0,)), ((), ()))


def mm(left, right, dims=NN):
    return lax.dot_general(left, right, dims, preferred_element_type=jnp.float32)


def block_scalars(meta_ref, block):
    leaf_side = meta_ref[0] == 1
    segment = jnp.where(leaf_side, block + (1 + NBRANCH), block - (TRUNK // SEG - 1))
    present = segment >= 1
    index = jnp.maximum(segment, 0)
    parent = meta_ref[1 + NSEG + index]
    own_count = jnp.where(present, meta_ref[1 + index], 0)
    parent_count = jnp.where(present & (parent >= 1), meta_ref[1 + parent], 0)
    parent_row = TRUNK + SEG * jnp.maximum(parent - 1, 0)
    return own_count, parent_count, pl.multiple_of(parent_row, SEG)


def trunk_limits(meta_ref, step):
    causal = (meta_ref[0] == 0) & (step < TRUNK // CHUNK)
    return meta_ref[1], jnp.where(causal, step * CHUNK, TRUNK)


def head_masks(dtype, value):
    lane = lax.broadcasted_iota(jnp.int32, (1, PAIR), 1)
    first = jnp.where(lane < E, value, 0.0).astype(dtype)
    second = jnp.where(lane < E, 0.0, value).astype(dtype)
    return first, second


def forward_kernel(meta_ref, q_ref, kv_ref, o_ref, lse_ref):
    step = pl.program_id(1)
    local_rows = kv_ref.shape[0] // 2
    query = q_ref[...]
    scale = head_masks(query.dtype, E ** (-0.5))
    trunk_count, shift = trunk_limits(meta_ref, step)
    key_pos = lax.broadcasted_iota(jnp.int32, (CHUNK, TRUNK), 1)
    row_pos = lax.broadcasted_iota(jnp.int32, (CHUNK, TRUNK), 0)
    trunk_ok = (key_pos <= row_pos + shift) & (key_pos < trunk_count)
    seg_key = lax.broadcasted_iota(jnp.int32, (SEG, SEG), 1)
    seg_row = lax.broadcasted_iota(jnp.int32, (SEG, SEG), 0)
    starts, par_ok, own_ok = [], [], []
    for j in range(CHUNK // SEG):
        block = step * (CHUNK // SEG) + j
        own_count, parent_count, parent_row = block_scalars(meta_ref, block)
        starts.append((parent_row, pl.multiple_of(local_rows + block * SEG, SEG)))
        par_ok.append(seg_key < parent_count)
        own_ok.append((seg_key <= seg_row) & (seg_key < own_count))
    outs, lses = [], []
    for h in range(2):
        qh = query * scale[h]
        trunk = jnp.where(trunk_ok, mm(qh, kv_ref[0:TRUNK, 0:PAIR], NT), NEG)
        par, own = [], []
        for j, (first, second) in enumerate(starts):
            qj = qh[j * SEG : (j + 1) * SEG]
            par.append(jnp.where(par_ok[j], mm(qj, kv_ref[pl.ds(first, SEG), 0:PAIR], NT), NEG))
            own.append(jnp.where(own_ok[j], mm(qj, kv_ref[pl.ds(second, SEG), 0:PAIR], NT), NEG))
        par_all = jnp.concatenate(par, axis=0)
        own_all = jnp.concatenate(own, axis=0)
        top = jnp.maximum(par_all, own_all)
        for i in range(TRUNK // SEG):
            top = jnp.maximum(top, trunk[:, i * SEG : (i + 1) * SEG])
        top = jnp.max(top, axis=1, keepdims=True)
        trunk = jnp.exp(trunk - top)
        par_all = jnp.exp(par_all - top)
        own_all = jnp.exp(own_all - top)
        total = par_all + own_all
        for i in range(TRUNK // SEG):
            total = total + trunk[:, i * SEG : (i + 1) * SEG]
        total = jnp.sum(total, axis=1, keepdims=True)
        out = mm(trunk.astype(jnp.bfloat16), kv_ref[0:TRUNK, PAIR : 2 * PAIR])
        tails = []
        for j, (first, second) in enumerate(starts):
            part = slice(j * SEG, (j + 1) * SEG)
            tails.append(
                mm(par_all[part].astype(jnp.bfloat16), kv_ref[pl.ds(first, SEG), PAIR : 2 * PAIR])
                + mm(own_all[part].astype(jnp.bfloat16), kv_ref[pl.ds(second, SEG), PAIR : 2 * PAIR])
            )
        out = out + jnp.concatenate(tails, axis=0)
        outs.append(out * (1.0 / total))
        lses.append(jnp.broadcast_to(top + jnp.log(total), (CHUNK, PAIR)))
    lane = lax.broadcasted_iota(jnp.int32, (CHUNK, PAIR), 1)
    o_ref[...] = jnp.where(lane < E, outs[0], outs[1]).astype(o_ref.dtype)
    turned = jnp.transpose(jnp.where(lane < E, lses[0], lses[1]))
    lse_ref[0, 0:1, :] = turned[0:1, :]
    lse_ref[0, 1:2, :] = turned[E : E + 1, :]


def attend_forward(meta, query, kv):
    rows, width = query.shape
    pairs = width // PAIR
    return pl.pallas_call(
        forward_kernel,
        grid_spec=pltpu.PrefetchScalarGridSpec(
            num_scalar_prefetch=1,
            grid=(pairs, rows // CHUNK),
            in_specs=[
                pl.BlockSpec((CHUNK, PAIR), lambda p, c, meta: (c, p)),
                pl.BlockSpec((2 * rows, 2 * PAIR), lambda p, c, meta: (0, p)),
            ],
            out_specs=[
                pl.BlockSpec((CHUNK, PAIR), lambda p, c, meta: (c, p)),
                pl.BlockSpec((1, 2, CHUNK), lambda p, c, meta: (p, 0, c)),
            ],
        ),
        out_shape=[
            jax.ShapeDtypeStruct((rows, width), jnp.bfloat16),
            jax.ShapeDtypeStruct((pairs, 2, rows), jnp.float32),
        ],
        name="attend_forward",
    )(meta, query, kv)


def backward_kernel(meta_ref, q_ref, kv_ref, o_ref, do_ref, lse_ref, dq_ref, dkv_ref, acc_ref):
    step = pl.program_id(1)
    local_rows = kv_ref.shape[0] // 2

    @pl.when(step == 0)
    def _():
        acc_ref[...] = jnp.zeros_like(acc_ref)

    query = q_ref[...]
    grad = do_ref[...]
    scale = head_masks(query.dtype, E ** (-0.5))
    keep = head_masks(query.dtype, 1.0)
    product = jnp.transpose(grad.astype(jnp.float32) * o_ref[...].astype(jnp.float32))
    trunk_count, shift = trunk_limits(meta_ref, step)
    key_pos = lax.broadcasted_iota(jnp.int32, (TRUNK, CHUNK), 0)
    row_pos = lax.broadcasted_iota(jnp.int32, (TRUNK, CHUNK), 1)
    trunk_ok = (key_pos <= row_pos + shift) & (key_pos < trunk_count)
    seg_key = lax.broadcasted_iota(jnp.int32, (SEG, SEG), 0)
    seg_row = lax.broadcasted_iota(jnp.int32, (SEG, SEG), 1)
    blocks = []
    for j in range(CHUNK // SEG):
        block = step * (CHUNK // SEG) + j
        own_count, parent_count, parent_row = block_scalars(meta_ref, block)
        own_row = pl.multiple_of(local_rows + block * SEG, SEG)
        blocks.append(
            (
                (parent_row, seg_key < parent_count),
                (own_row, (seg_key <= seg_row) & (seg_key < own_count)),
            )
        )
    query_grads = []
    trunk_parts = []
    block_parts = [[[], []] for _ in blocks]
    for h in range(2):
        qh = query * scale[h]
        gh = grad * keep[h]
        lse = lse_ref[0, h : h + 1, :]
        inner = jnp.sum(product[h * E : (h + 1) * E], axis=0, keepdims=True)

        def part(rows, allowed, qs, gs, lse_row, inner_row):
            keys = kv_ref[rows, 0:PAIR]
            values = kv_ref[rows, PAIR : 2 * PAIR]
            scores = jnp.where(allowed, mm(keys, qs, NT), NEG)
            probs = jnp.exp(scores - lse_row)
            score_grad = (probs * (mm(values, gs, NT) - inner_row)).astype(jnp.bfloat16)
            return (
                mm(score_grad, keys, TN),
                mm(score_grad, qs),
                mm(probs.astype(jnp.bfloat16), gs),
            )

        query_grad, key_part, value_part = part(slice(0, TRUNK), trunk_ok, qh, gh, lse, inner)
        trunk_parts.append((key_part, value_part))
        tails = []
        for j, sources in enumerate(blocks):
            cut = slice(j * SEG, (j + 1) * SEG)
            tail = 0.0
            for k, (first, allowed) in enumerate(sources):
                moved, key_part, value_part = part(
                    pl.ds(first, SEG), allowed, qh[cut], gh[cut], lse[:, cut], inner[:, cut]
                )
                tail = tail + moved
                block_parts[j][k].append((key_part, value_part))
            tails.append(tail)
        query_grads.append(query_grad + jnp.concatenate(tails, axis=0))
    lane = lax.broadcasted_iota(jnp.int32, (CHUNK, PAIR), 1)
    dq_ref[...] = (jnp.where(lane < E, query_grads[0], query_grads[1]) * E ** (-0.5)).astype(
        dq_ref.dtype
    )
    for side in range(2):
        cols = slice(side * PAIR, (side + 1) * PAIR)
        acc_ref[0:TRUNK, cols] += trunk_parts[0][side] + trunk_parts[1][side]
        for j, sources in enumerate(blocks):
            for k, (first, _) in enumerate(sources):
                both = block_parts[j][k][0][side] + block_parts[j][k][1][side]
                if k == 0:
                    acc_ref[pl.ds(first, SEG), cols] += both
                else:
                    dkv_ref[pl.ds(first, SEG), cols] = both.astype(dkv_ref.dtype)

    @pl.when(step == pl.num_programs(1) - 1)
    def _():
        dkv_ref[0:local_rows, :] = acc_ref[...].astype(dkv_ref.dtype)


def attend_backward(meta, query, kv, out, grad, lse):
    rows, width = query.shape
    pairs = width // PAIR
    row_spec = pl.BlockSpec((CHUNK, PAIR), lambda p, c, meta: (c, p))
    kv_spec = pl.BlockSpec((2 * rows, 2 * PAIR), lambda p, c, meta: (0, p))
    return pl.pallas_call(
        backward_kernel,
        grid_spec=pltpu.PrefetchScalarGridSpec(
            num_scalar_prefetch=1,
            grid=(pairs, rows // CHUNK),
            in_specs=[
                row_spec,
                kv_spec,
                row_spec,
                row_spec,
                pl.BlockSpec((1, 2, CHUNK), lambda p, c, meta: (p, 0, c)),
            ],
            out_specs=[row_spec, kv_spec],
            scratch_shapes=[pltpu.VMEM((rows, 2 * PAIR), jnp.float32)],
        ),
        out_shape=[
            jax.ShapeDtypeStruct((rows, width), jnp.bfloat16),
            jax.ShapeDtypeStruct((2 * rows, 2 * width), jnp.bfloat16),
        ],
        name="attend_backward",
    )(meta, query, kv, out, grad, lse)


def norm_stats(inputs):
    inverse = lax.rsqrt(jnp.mean(inputs * inputs, axis=-1, keepdims=True) + EPSILON)
    return (inputs * inverse, inverse)


def norm_back(normed_grad, gain_vec, normed, inverse):
    scaled = normed_grad * gain_vec
    inner = jnp.mean(scaled * normed, axis=-1, keepdims=True)
    return (inverse * (scaled - normed * inner), jnp.sum(normed_grad * normed, axis=0))


def interleave(keys, values):
    rows, width = keys.shape
    shape = (rows, width // PAIR, 1, PAIR)
    both = jnp.concatenate([keys.reshape(shape), values.reshape(shape)], axis=2)
    return both.reshape(rows, 2 * width)


def swap_sides(array):
    return lax.ppermute(array, "tensor", [(0, 1), (1, 0)])


def all_sum(array):
    array = array + swap_sides(array)
    size = lax.axis_size("dp")
    step = 1
    while step < size:
        array = array + lax.ppermute(array, "dp", [(i, i ^ step) for i in range(size)])
        step *= 2
    return array


def local(
    layer_input,
    gain_attn,
    w_query,
    w_latent,
    w_key,
    w_value,
    w_output,
    gain_ffn,
    w_gate,
    w_up,
    w_down,
    parents,
    counts,
    upstream_grad,
):
    bf16 = jnp.bfloat16
    row_count, model_width = layer_input.shape
    sides = lax.axis_size("tensor")
    dp_size = lax.axis_size("dp")
    side = lax.axis_index("tensor")
    shard_rows, query_len = w_query.shape
    latent_len = w_latent.shape[1]
    hidden_len = w_gate.shape[1]
    kv_rows, kv_len = w_key.shape[1:]
    gain_len = gain_attn.shape[0]
    kv_cols = kv_rows * 2 * kv_len // shard_rows
    gain_cols = 2 * E

    meta = jnp.concatenate([side[None].astype(jnp.int32), counts[0], parents[0]])

    sent = lax.ppermute(layer_input, "tensor", [(0, 1)])

    gain_row = jnp.concatenate([gain_attn, gain_ffn])[None, :]
    gain_block = jnp.pad(gain_row, ((0, shard_rows - 1), (0, gain_cols - 2 * gain_len)))
    attn_pack = jnp.concatenate(
        [
            w_query,
            w_latent,
            w_output.T,
            interleave(w_key[0], w_value[0]).reshape(shard_rows, kv_cols),
            gain_block,
        ],
        axis=1,
    )
    attn_all = lax.all_gather(attn_pack, GATHER_AXES, axis=0, tiled=True)
    ffn_pack = jnp.concatenate([w_gate, w_up, w_down.T], axis=1)
    ffn_all = lax.all_gather(ffn_pack, GATHER_AXES, axis=0, tiled=True)

    owners = [1 - side, side]

    def half_of(gathered, u, first, size):
        return lax.dynamic_slice(gathered, (owners[u] * model_width, first), (model_width, size))

    first_latent = query_len
    first_out = first_latent + latent_len
    first_kv = first_out + query_len
    first_gain = first_kv + kv_cols
    query_w = [half_of(attn_all, u, 0, query_len) for u in range(2)]
    latent_w = [half_of(attn_all, u, first_latent, latent_len) for u in range(2)]
    out_w = [half_of(attn_all, u, first_out, query_len) for u in range(2)]
    kv_w = [
        half_of(attn_all, u, first_kv, kv_cols).reshape(dp_size * kv_rows, 2 * kv_len)
        for u in range(2)
    ]
    gains = attn_all[:, first_gain : first_gain + 2 * gain_len]
    gains = gains.reshape(sides, dp_size, shard_rows, 2, gain_len)[:, :, 0]
    gains = gains.transpose(2, 1, 0, 3).reshape(2, model_width).astype(jnp.float32)
    gain_one, gain_two = gains[0], gains[1]
    gate_w = [half_of(ffn_all, u, 0, hidden_len) for u in range(2)]
    up_w = [half_of(ffn_all, u, hidden_len, hidden_len) for u in range(2)]
    down_w = [half_of(ffn_all, u, 2 * hidden_len, hidden_len) for u in range(2)]

    context_input = jnp.where(side == 0, layer_input, sent)
    inputs = layer_input.astype(jnp.float32)
    normed_one, inverse_one = norm_stats(inputs)
    attn_in = (normed_one * gain_one).astype(bf16)
    context_in = (norm_stats(context_input.astype(jnp.float32))[0] * gain_one).astype(bf16)
    both_in = jnp.concatenate([context_in, attn_in], axis=0)
    queries, latents, kvs, heads, lses = [], [], [], [], []
    for u in range(2):
        latents.append(mm(both_in, latent_w[u]).astype(bf16))
        queries.append(mm(attn_in, query_w[u]).astype(bf16))
        kvs.append(mm(latents[u], kv_w[u]).astype(bf16))
        out, lse = attend_forward(meta, queries[u], kvs[u])
        heads.append(out)
        lses.append(lse)
    branch = mm(heads[0], out_w[0], NT) + mm(heads[1], out_w[1], NT)
    residual = inputs + branch
    normed_two, inverse_two = norm_stats(residual)
    ffn_in = (normed_two * gain_two).astype(bf16)

    def half_grad(left, rights):
        received = swap_sides(mm(left, rights[0], TN).astype(bf16))
        return lambda: (mm(left, rights[1], TN) + received.astype(jnp.float32)).astype(bf16)

    gates = [mm(ffn_in, gate_w[u]) for u in range(2)]
    ups = [mm(ffn_in, up_w[u]) for u in range(2)]
    sigs = [jax.nn.sigmoid(gate) for gate in gates]
    hiddens = [(gates[u] * sigs[u] * ups[u]).astype(bf16) for u in range(2)]

    first_cols = [0, hidden_len, 2 * hidden_len, 3 * hidden_len]
    first_pack = jnp.zeros((sides * model_width, 3 * hidden_len + query_len), bf16)

    def put(pack, k, u, value):
        return lax.dynamic_update_slice(
            pack, value.astype(bf16), (owners[u] * model_width, first_cols[k])
        )

    for u in range(2):
        first_pack = put(first_pack, 0, u, mm(upstream_grad, hiddens[u], TN))
    ffn_out = mm(hiddens[0], down_w[0], NT) + mm(hiddens[1], down_w[1], NT)
    final_out = (residual + ffn_out).astype(bf16)

    position = side * row_count + lax.broadcasted_iota(jnp.int32, (row_count, NSEG), 0)
    seg_ids = lax.broadcasted_iota(jnp.int32, (row_count, NSEG), 1)
    beyond = position - TRUNK
    segment = jnp.where(beyond < 0, 0, 1 + beyond // SEG)
    offset = jnp.where(beyond < 0, position, beyond % SEG)
    valid = jnp.any((segment == seg_ids) & (offset < counts[0][None, :]), axis=1, keepdims=True)
    valid = valid.astype(jnp.float32)
    stat_terms = jnp.stack(
        [
            jnp.sum(valid * branch * branch),
            jnp.sum(valid * residual * residual),
            jnp.sum(valid * ffn_out * ffn_out),
            jnp.sum(valid),
        ]
    )

    normed_grad_two = 0.0
    for u in range(2):
        hidden_grad = mm(upstream_grad, down_w[u])
        gate_act = gates[u] * sigs[u]
        gate_grad = (
            hidden_grad * ups[u] * sigs[u] * (1.0 + gates[u] * (1.0 - sigs[u]))
        ).astype(bf16)
        up_grad = (hidden_grad * gate_act).astype(bf16)
        normed_grad_two = (
            normed_grad_two + mm(gate_grad, gate_w[u], NT) + mm(up_grad, up_w[u], NT)
        )
        first_pack = put(first_pack, 1, u, mm(ffn_in, gate_grad, TN))
        first_pack = put(first_pack, 2, u, mm(ffn_in, up_grad, TN))
    residual_part, gain_two_grad = norm_back(normed_grad_two, gain_two, normed_two, inverse_two)
    residual_grad = upstream_grad.astype(jnp.float32) + residual_part
    branch_grad = residual_grad.astype(bf16)
    for u in range(2):
        first_pack = put(first_pack, 3, u, mm(branch_grad, heads[u], TN))
    first_pack, branch_grad = lax.optimization_barrier((first_pack, branch_grad))
    ffn_sum = lax.psum_scatter(first_pack, GATHER_AXES, scatter_dimension=0, tiled=True)

    query_grads, kv_grads, latent_parts = [], [], []
    for u in range(2):
        heads_grad = mm(branch_grad, out_w[u]).astype(bf16)
        if u == 1:
            query_out = mm(attn_in, query_grads[0], TN).astype(bf16)
            kv_out = mm(latents[0], kv_grads[0], TN).astype(bf16)
            query_out, kv_out, heads_grad = lax.optimization_barrier(
                (query_out, kv_out, heads_grad)
            )
            query_in = swap_sides(query_out)
            kv_in = swap_sides(kv_out)
        query_grad, kv_grad = attend_backward(
            meta, queries[u], kvs[u], heads[u], heads_grad, lses[u]
        )
        query_grads.append(query_grad)
        kv_grads.append(kv_grad)
        latent_parts.append(mm(kv_grad, kv_w[u], NT))
    query_half = (mm(attn_in, query_grads[1], TN) + query_in.astype(jnp.float32)).astype(bf16)
    kv_half = (mm(latents[1], kv_grads[1], TN) + kv_in.astype(jnp.float32)).astype(bf16)
    latent_grads = []
    for u in range(2):
        returned = lax.ppermute(
            latent_parts[1 - u][:row_count].astype(bf16), "tensor", [(1, 0)]
        )
        latent_grads.append(
            (
                latent_parts[u][row_count:]
                + jnp.where(side == 0, latent_parts[u][:row_count], 0.0)
                + returned.astype(jnp.float32)
            ).astype(bf16)
        )
    latent_half = half_grad(attn_in, latent_grads)
    attn_pack = jnp.concatenate(
        [query_half, latent_half(), kv_half.reshape(model_width, kv_cols)], axis=1
    )
    attn_pack, ffn_sum = lax.optimization_barrier((attn_pack, ffn_sum))
    attn_sum = lax.psum_scatter(attn_pack, "dp", scatter_dimension=0, tiled=True)
    attn_sum = attn_sum.astype(jnp.float32)
    normed_grad_one = (
        mm(query_grads[0], query_w[0], NT)
        + mm(query_grads[1], query_w[1], NT)
        + mm(latent_grads[0], latent_w[0], NT)
        + mm(latent_grads[1], latent_w[1], NT)
    )
    input_part, gain_one_grad = norm_back(normed_grad_one, gain_one, normed_one, inverse_one)
    input_grad = residual_grad + input_part

    stat_row = jnp.pad(stat_terms, (0, 8 * 2 * E - 4))
    totals = all_sum(
        jnp.concatenate([gain_one_grad, gain_two_grad, stat_row]).reshape(-1, 2 * E)
    ).reshape(-1)
    own_start = lax.axis_index(("dp", "tensor")) * gain_len
    stat_totals = totals[2 * model_width : 2 * model_width + 4]
    rms_stats = jnp.sqrt(stat_totals[:3] / (stat_totals[3] * model_width))
    kv_sum = attn_sum[:, first_out : first_out + kv_cols].reshape(
        kv_rows, kv_len // PAIR, 2, PAIR
    )
    ffn_sum = ffn_sum.astype(jnp.float32)
    return (
        final_out,
        input_grad,
        lax.dynamic_slice_in_dim(totals, own_start, gain_len),
        attn_sum[:, :query_len],
        attn_sum[:, first_latent:first_out],
        kv_sum[:, :, 0].reshape(1, kv_rows, kv_len),
        kv_sum[:, :, 1].reshape(1, kv_rows, kv_len),
        ffn_sum[:, 3 * hidden_len :].T,
        lax.dynamic_slice_in_dim(totals, model_width + own_start, gain_len),
        ffn_sum[:, hidden_len : 2 * hidden_len],
        ffn_sum[:, 2 * hidden_len : 3 * hidden_len],
        ffn_sum[:, :hidden_len].T,
        rms_stats,
    )


def solution(mesh):
    placed = (
        P(("dp", "tensor"), None),
        P(("dp", "tensor")),
        P("dp", "tensor"),
        P("dp", "tensor"),
        P("tensor", "dp", None),
        P("tensor", "dp", None),
        P("tensor", "dp"),
        P(("dp", "tensor")),
        P("dp", "tensor"),
        P("dp", "tensor"),
        P("tensor", "dp"),
        P("dp", None),
        P("dp", None),
        P(("dp", "tensor"), None),
    )
    return jax.shard_map(
        local,
        mesh=mesh,
        in_specs=placed,
        out_specs=(
            P(("dp", "tensor"), None),
            P(("dp", "tensor"), None),
            P(("dp", "tensor")),
            P("dp", "tensor"),
            P("dp", "tensor"),
            P("tensor", "dp", None),
            P("tensor", "dp", None),
            P("tensor", "dp"),
            P(("dp", "tensor")),
            P("dp", "tensor"),
            P("dp", "tensor"),
            P("tensor", "dp"),
            P(),
        ),
        check_vma=False,
    )
```
